32 devices in a mesh: data: 1 (over z), model: 4 (over y), seq: 8 (over x, core).
Axes of the slice: x: 4, y: 4, z: 1, core: 2. Of those that a mesh axis runs over, the one named last changes fastest.
The devices are a block of a 4x4x8 slice.
Arguments:
- tokens: bfloat16 [64, 4096, 768], P('data', 'seq')
- lengths: int32 [64], P('data')
- slot_params: bfloat16 [768, 128], replicated
- logit_scale: float32 [], replicated
- w_in: bfloat16 [32, 768, 3072], P('seq', None, 'model')
- w_out: bfloat16 [32, 3072, 768], P('seq', 'model')
Outputs:
- output: bfloat16 [64, 4096, 768], P('data', 'seq')
All inputs are finite; a program needn't handle non-finite values.
Results may differ from the reference program's by a relative error of at most 0.0153139.
Values are sent between devices in bfloat16 or wider.
A program may use at most 768 MiB of HBM per device.

```python
import math
import jax
import jax.numpy as jnp
from jax import lax

BATCH_SIZE = 64
SEQ_LEN = 4096
MODEL_DIM = 768
HIDDEN_DIM = 3072
NUM_EXPERTS = 32
EXPERT_SLOTS = 4
NUM_SLOTS_TOTAL = NUM_EXPERTS * EXPERT_SLOTS
NORM_EPS = 1e-6


def setup_inputs(seed: int = 0, part: int = 0) -> dict:
    root_key = jax.random.key(seed)
    key_phi, key_gain, key_win, key_wout, key_part = jax.random.split(root_key, 5)
    part_key = jax.random.fold_in(key_part, part)
    key_tok, key_len = jax.random.split(part_key, 2)
    tokens = jax.random.normal(key_tok, (BATCH_SIZE, SEQ_LEN, MODEL_DIM), jnp.float32).astype(jnp.bfloat16)
    drawn = jax.random.randint(key_len, (BATCH_SIZE,), SEQ_LEN // 4, SEQ_LEN + 1, jnp.int32)
    lengths = jnp.where(jnp.arange(BATCH_SIZE) == 0, SEQ_LEN, drawn).astype(jnp.int32)
    slot_params = jax.random.normal(key_phi, (MODEL_DIM, NUM_SLOTS_TOTAL), jnp.float32).astype(jnp.bfloat16)
    logit_scale = math.sqrt(MODEL_DIM) * jax.random.uniform(key_gain, (), jnp.float32, 1.0, 2.0)
    in_scale = math.sqrt(SEQ_LEN) / (4.0 * math.sqrt(MODEL_DIM))
    w_in = (jax.random.normal(key_win, (NUM_EXPERTS, MODEL_DIM, HIDDEN_DIM), jnp.float32) * in_scale).astype(jnp.bfloat16)
    w_out = (jax.random.normal(key_wout, (NUM_EXPERTS, HIDDEN_DIM, MODEL_DIM), jnp.float32) / math.sqrt(HIDDEN_DIM)).astype(jnp.bfloat16)
    return {"tokens": tokens, "lengths": lengths, "slot_params": slot_params, "logit_scale": logit_scale, "w_in": w_in, "w_out": w_out}


def unit_vectors(values, axis):
    v32 = values.astype(jnp.float32)
    return (v32 * lax.rsqrt(jnp.sum(v32 * v32, axis=axis, keepdims=True) + NORM_EPS)).astype(jnp.bfloat16)


def reference(tokens, lengths, slot_params, logit_scale, w_in, w_out):
    slot_unit = unit_vectors(slot_params, 0)
    positions = jnp.arange(SEQ_LEN)

    def seq_logits(seq_tokens):
        return logit_scale * jnp.dot(unit_vectors(seq_tokens, 1), slot_unit, preferred_element_type=jnp.float32)

    def dispatch(args):
        seq_tokens, seq_length = args
        logits = seq_logits(seq_tokens)
        masked = jnp.where((positions < seq_length)[:, None], logits, -1e30)
        weights = jnp.exp(masked - jnp.max(masked, axis=0, keepdims=True))
        col_sum = jnp.sum(weights, axis=0)
        slot_sum = jnp.dot(weights.astype(jnp.bfloat16).T, seq_tokens, preferred_element_type=jnp.float32)
        return (slot_sum / col_sum[:, None]).astype(jnp.bfloat16)

    slot_in = lax.map(dispatch, (tokens, lengths))
    per_expert = slot_in.reshape(BATCH_SIZE, NUM_EXPERTS, EXPERT_SLOTS, MODEL_DIM).transpose(1, 0, 2, 3).reshape(NUM_EXPERTS, BATCH_SIZE * EXPERT_SLOTS, MODEL_DIM)

    def expert_ffn(args):
        rows, first, second = args
        hidden = jax.nn.gelu(jnp.dot(rows, first, preferred_element_type=jnp.float32), approximate=False).astype(jnp.bfloat16)
        return jnp.dot(hidden, second, preferred_element_type=jnp.float32).astype(jnp.bfloat16)

    expert_out = lax.map(expert_ffn, (per_expert, w_in, w_out))
    slot_out = expert_out.reshape(NUM_EXPERTS, BATCH_SIZE, EXPERT_SLOTS, MODEL_DIM).transpose(1, 0, 2, 3).reshape(BATCH_SIZE, NUM_SLOTS_TOTAL, MODEL_DIM)

    def combine(args):
        seq_tokens, seq_length, seq_slots = args
        mix_weights = jax.nn.softmax(seq_logits(seq_tokens), axis=1).astype(jnp.bfloat16)
        mixed = jnp.dot(mix_weights, seq_slots, preferred_element_type=jnp.float32)
        return jnp.where((positions < seq_length)[:, None], mixed, 0.0).astype(jnp.bfloat16)

    return lax.map(combine, (tokens, lengths, slot_out))
```

```python
import functools

import jax
import jax.numpy as jnp
import numpy as np
from jax import lax
from jax.experimental import pallas as pl
from jax.experimental.pallas import tpu as pltpu
from jax.sharding import PartitionSpec as P

NORM_EPS = 1e-6
NEG = -1e30
MESH = pl.DeviceIdType.MESH
CORES = 2
RING = 4
CHUNKS = 2
TOK_BUFS = 3
VMEM_LIMIT = 60 * 1024 * 1024


def unit_vectors(values, axis):
    v32 = values.astype(jnp.float32)
    return (v32 * lax.rsqrt(jnp.sum(v32 * v32, axis=axis, keepdims=True) + NORM_EPS)).astype(jnp.bfloat16)


def scaled_logits(x, v, g):
    return g * jnp.dot(unit_vectors(x, 1), v, preferred_element_type=jnp.float32)


def row_softmax(logits):
    e = jnp.exp(logits - jnp.max(logits, axis=1, keepdims=True))
    return (e * (1.0 / jnp.sum(e, axis=1, keepdims=True))).astype(jnp.bfloat16)


def dispatch_kernel(pos_ref, len_ref, g_ref, x_ref, v_ref, s_ref, mz_ref, c_ref):
    i = pl.program_id(0)
    group, toks = s_ref.shape[0], x_ref.shape[1]
    del group
    x = x_ref[0]
    logits = scaled_logits(x, v_ref[...], g_ref[0])
    c_ref[0] = row_softmax(logits)
    first = pos_ref[1] * toks
    length = len_ref[pos_ref[0] * pl.num_programs(0) + i]
    valid = first + lax.broadcasted_iota(jnp.int32, logits.shape, 0) < length
    masked = jnp.where(valid, logits, NEG)
    top = jnp.max(masked, axis=0, keepdims=True)
    w = jnp.where(valid, jnp.exp(masked - top), 0.0)
    mz_ref[0, pl.ds(i, 1), :] = top
    mz_ref[1, pl.ds(i, 1), :] = jnp.sum(w, axis=0, keepdims=True)
    s_ref[0] = lax.dot_general(w.astype(jnp.bfloat16), x, (((0,), (0,)), ((), ())), preferred_element_type=jnp.float32).astype(jnp.bfloat16)


def exchange_kernel(dims, plan, tok_hbm, g_ref, v_ref, s_hbm, mz_ref, win_hbm, wout_hbm, perm_ref, permt_ref,
                    ysa_hbm, ysb_hbm, c_hbm,
                    tokbuf, cbuf, s_buf, mz_all, win, wout, sc, dr, pb, fx, sx, rx, xs, op, fy, sy, ry, ysa, ysb,
                    tok_sem, c_sem, load_sem, out_sem, send_sem, recv_sem):
    chunks, bc, n_seq, group, n_fill, slots = dims
    bh, bq = bc // 2, bc // 4
    n = bc * slots
    m, s = lax.axis_index("model"), lax.axis_index("seq")
    c, x = lax.rem(s, CORES), lax.div(s, CORES)
    oc = 1 - c
    xr, xl, xo = lax.rem(x + 1, RING), lax.rem(x + RING - 1, RING), lax.rem(x + 2, RING)
    mr, ml, mo = lax.rem(m + 1, RING), lax.rem(m + RING - 1, RING), lax.rem(m + 2, RING)
    right, left = {"seq": xr * CORES + c}, {"seq": xl * CORES + c}
    up, down = {"model": mr}, {"model": ml}
    twin = {"seq": x * CORES + oc}
    row_peers = [{"seq": lax.rem(s + d, n_seq)} for d in range(1, n_seq)]
    peers = row_peers + [up, down]

    loads = [pltpu.make_async_copy(a, b, load_sem.at[i]) for i, (a, b) in enumerate(((s_hbm, s_buf), (win_hbm, win), (wout_hbm, wout)))]
    for ld in loads:
        ld.start()
    batch = tok_hbm.shape[0]

    def tok_copy(i):
        b = lax.rem((m + 1) * group + i, batch)
        slot = lax.rem(i, TOK_BUFS)
        return pltpu.make_async_copy(tok_hbm.at[b], tokbuf.at[slot], tok_sem.at[slot])

    def c_copy(i):
        slot = lax.rem(i, 2)
        return pltpu.make_async_copy(cbuf.at[slot], c_hbm.at[i], c_sem.at[slot])

    for i in range(TOK_BUFS - 1):
        tok_copy(jnp.int32(i)).start()

    barrier = pltpu.get_barrier_semaphore()
    for peer in peers:
        pl.semaphore_signal(barrier, inc=1, device_id=peer, device_id_type=MESH)
    pl.semaphore_wait(barrier, len(peers))

    copies = []

    def send(src, dst, dev):
        i = len(copies)
        d = pltpu.make_async_remote_copy(src_ref=src, dst_ref=dst, send_sem=send_sem.at[i], recv_sem=recv_sem.at[i], device_id=dev, device_id_type=MESH)
        d.start()
        copies.append(d)
        return d

    mz_sends = [send(mz_ref, mz_all.at[s], peer) for peer in row_peers]
    mz_all[s] = mz_ref[...]

    filled = [0]

    def fill(count):
        lo = filled[0]
        hi = min(lo + count, n_fill)
        filled[0] = hi
        if hi == lo:
            return

        def one(i, carry):
            tok_copy(i).wait()

            @pl.when(i + TOK_BUFS - 1 < n_fill)
            def _():
                tok_copy(i + TOK_BUFS - 1).start()

            @pl.when(i >= 2)
            def _():
                c_copy(i).wait()

            cbuf[lax.rem(i, 2)] = row_softmax(scaled_logits(tokbuf[lax.rem(i, TOK_BUFS)], v_ref[...], g_ref[0]))
            c_copy(i).start()
            return carry

        lax.fori_loop(lo, hi, one, 0)

    state = {}

    def factor():
        for d in mz_sends:
            d.wait_recv()
        tops = [mz_all[q, 0] for q in range(n_seq)]
        top = functools.reduce(jnp.maximum, tops)
        z = functools.reduce(jnp.add, [mz_all[q, 1] * jnp.exp(tops[q] - top) for q in range(n_seq)])
        state["f"] = jnp.transpose(jnp.exp(mz_ref[0] - top) / z)
        loads[0].wait()

    def scale(k):
        for j in range(bc):
            b = k * bc + j
            val = s_buf[b].astype(jnp.float32) * state["f"][:, b:b + 1]
            val = val.astype(jnp.bfloat16)
            for q in range(n_seq):
                sc[k, q % CORES, j, q // CORES] = val[q * slots:(q + 1) * slots]
        state["d2d", k] = send(sc.at[k, oc], dr.at[k], twin)

    def ring_send(tag, k, buf, far, r, l, f, rcv, size, rdev, ldev):
        lo, hi = pl.ds(0, size // 2), pl.ds(size // 2, size // 2)
        state[tag, k, 0] = (send(buf.at[k, far, lo], f.at[k, 0], rdev), send(buf.at[k, far, hi], f.at[k, 1], ldev))
        state[tag, k, 1] = [send(buf.at[k, r, hi], rcv.at[k, 0, hi], rdev), send(buf.at[k, l, lo], rcv.at[k, 1, lo], ldev)]

    def ring_relay(tag, k, buf, r, l, f, relay, rcv, size, rdev, ldev):
        half = size // 2
        lo, hi = pl.ds(0, half), pl.ds(half, half)
        for d in state[tag, k, 0]:
            d.wait_recv()
        relay[k, 0] = (buf[k, r, lo].astype(jnp.float32) + f[k, 0].astype(jnp.float32)).astype(jnp.bfloat16)
        relay[k, 1] = (buf[k, l, hi].astype(jnp.float32) + f[k, 1].astype(jnp.float32)).astype(jnp.bfloat16)
        state[tag, k, 1] += [send(relay.at[k, 0], rcv.at[k, 0, lo], rdev), send(relay.at[k, 1], rcv.at[k, 1, hi], ldev)]

    def ring_sum(tag, k, own, rcv):
        for d in state[tag, k, 1]:
            d.wait_recv()
        return (own.astype(jnp.float32) + rcv[k, 0].astype(jnp.float32) + rcv[k, 1].astype(jnp.float32)).astype(jnp.bfloat16)

    def pair(k):
        state["d2d", k].wait_recv()
        for q in range(RING):
            pb[k, q] = (sc[k, c, :, q].astype(jnp.float32) + dr[k, :, q].astype(jnp.float32)).astype(jnp.bfloat16)
        ring_send("x", k, pb, xo, xr, xl, fx, rx, bc, right, left)

    def rsx2(k):
        ring_relay("x", k, pb, xr, xl, fx, sx, rx, bc, right, left)

    def slot_in(k):
        val = ring_sum("x", k, pb[k, x], rx).reshape(n, -1)
        xs[k, m] = jnp.dot(perm_ref[...], val, preferred_element_type=jnp.float32).astype(jnp.bfloat16)
        state["gy", k] = [send(xs.at[k, m], xs.at[k, m], dev) for dev in (up, down)]

    def gy2(k):
        for d in state["gy", k]:
            d.wait_recv()
        lo, hi = pl.ds(0, n // 2), pl.ds(n // 2, n // 2)
        state["gy2", k] = [send(xs.at[k, ml, lo], xs.at[k, ml, lo], up), send(xs.at[k, mr, hi], xs.at[k, mr, hi], down)]

    def experts(k):
        if k == 0:
            loads[1].wait()
            loads[2].wait()
        for d in state["gy2", k]:
            d.wait_recv()
        n_exp = win.shape[0]
        r = n // n_exp
        for e in range(n_exp):
            rows = xs[k, :, e * r:(e + 1) * r, :].reshape(RING * r, -1)
            h = jnp.dot(rows, win[e], preferred_element_type=jnp.float32)
            h = (0.5 * h * (1.0 + lax.erf(h * np.float32(np.sqrt(0.5))))).astype(jnp.bfloat16)
            o = jnp.dot(h, wout[e], preferred_element_type=jnp.float32).astype(jnp.bfloat16)
            op[k, :, e * r:(e + 1) * r, :] = o.reshape(RING, r, -1)
        ring_send("y", k, op, mo, mr, ml, fy, ry, n, up, down)

    def rsy2(k):
        ring_relay("y", k, op, mr, ml, fy, sy, ry, n, up, down)

    def slot_out(k):
        val = ring_sum("y", k, op[k, m], ry)
        val = jnp.dot(permt_ref[...], val, preferred_element_type=jnp.float32).astype(jnp.bfloat16).reshape(bc, slots, -1)
        ysa[k, x, c, m] = val[:bh]
        ysb[k, m, c, x] = val[bh:]
        a, b = ysa.at[k, x, c, m], ysb.at[k, m, c, x]
        state["g1", k] = [send(a, a, up), send(a, a, down), send(b, b, right), send(b, b, left)]

    def ag2(k):
        for d in state["g1", k]:
            d.wait_recv()
        lo, hi = pl.ds(0, bq), pl.ds(bq, bq)
        todo = [(ysa.at[k, x, c, ml, lo], up), (ysa.at[k, x, c, mr, hi], down), (ysb.at[k, m, c, xl, lo], right), (ysb.at[k, m, c, xr, hi], left)]
        state["g2", k] = [send(r, r, dev) for r, dev in todo]

    def ag3(k):
        for d in state["g2", k]:
            d.wait_recv()
        a, b = ysa.at[k, x, c], ysb.at[k, m, c]
        state["g3", k] = [send(a, a, right), send(a, a, left), send(b, b, up), send(b, b, down)]
        state["t", k] = [send(a, a, twin), send(b, b, twin)]

    def ag4(k):
        for d in state["g3", k]:
            d.wait_recv()
        lo, hi = pl.ds(0, RING // 2), pl.ds(RING // 2, RING // 2)
        todo = [(ysa.at[k, xl, c, lo], right), (ysa.at[k, xr, c, hi], left), (ysb.at[k, ml, c, lo], up), (ysb.at[k, mr, c, hi], down)]
        state["g4", k] = [send(r, r, dev) for r, dev in todo]
        state["t", k] += [send(r, r, twin) for r in (ysa.at[k, xl, c], ysa.at[k, xr, c], ysb.at[k, ml, c], ysb.at[k, mr, c])]

    def ag5(k):
        for d in state["g4", k]:
            d.wait_recv()
        state["t", k] += [send(r, r, twin) for r in (ysa.at[k, xo, c], ysb.at[k, mo, c])]

    outs = []

    def finish(k):
        for d in state["t", k]:
            d.wait_recv()
        for i, (a, b) in enumerate(((ysa, ysa_hbm), (ysb, ysb_hbm))):
            d = pltpu.make_async_copy(a.at[k], b.at[k], out_sem.at[2 * k + i])
            d.start()
            outs.append(d)

    stages = {f.__name__: f for f in (scale, pair, rsx2, slot_in, gy2, experts, rsy2, slot_out, ag2, ag3, ag4, ag5, finish)}
    for name, arg in plan:
        if name == "fill":
            fill(arg)
        elif name == "factor":
            factor()
        else:
            stages[name](arg)
    fill(n_fill)
    for d in outs:
        d.wait()
    for d in copies:
        d.wait_send()
    c_copy(jnp.int32(0)).wait()
    c_copy(jnp.int32(1)).wait()


STAGES = ("scale", "pair", "rsx2", "slot_in", "gy2", "experts", "rsy2", "slot_out", "ag2", "ag3", "ag4", "ag5", "finish")


def make_plan(chunks, n_fill):
    ticks = chunks + len(STAGES) - 1
    plan = [("fill", max(1, n_fill // 12)), ("factor", 0)]
    per = -(-(n_fill - n_fill // 12) // max(1, ticks - 4))
    for t in range(ticks):
        for st in reversed(range(len(STAGES))):
            if 0 <= t - st < chunks:
                plan.append((STAGES[st], t - st))
        plan.append(("fill", per))
    return tuple(plan)


def combine_kernel(pos_ref, len_ref, c0_ref, c1_ref, ysa_ref, ysb_ref, y_ref):
    r, k, h = pl.program_id(0), pl.program_id(1), pl.program_id(2)
    bh, toks = y_ref.shape[0], y_ref.shape[1]
    group = pl.num_programs(1) * 2 * bh
    base = lax.rem(pos_ref[0] + r, RING) * group + (k * 2 + h) * bh
    first = pos_ref[1] * toks

    def emit(c_ref, table):
        for j in range(bh):
            mixed = jnp.dot(c_ref[j], table(j), preferred_element_type=jnp.float32)
            valid = first + lax.broadcasted_iota(jnp.int32, mixed.shape, 0) < len_ref[base + j]
            y_ref[j] = jnp.where(valid, mixed, 0.0).astype(y_ref.dtype)

    def table_a(j):
        return ysa_ref[0, :, :, 0, j].reshape(-1, y_ref.shape[2])

    def table_b(j):
        return jnp.concatenate([ysb_ref[0, 0, q % CORES, q // CORES, j] for q in range(CORES * RING)], axis=0)

    for first_group, c_ref in ((True, c0_ref), (False, c1_ref)):
        for half, table in ((0, table_a), (1, table_b)):
            @pl.when(((r == 0) == first_group) & (h == half))
            def _(c_ref=c_ref, table=table):
                emit(c_ref, table)


def solution(mesh):
    n_seq, n_model = mesh.shape["seq"], mesh.shape["model"]
    assert n_model == RING and n_seq == RING * CORES

    def local_layer(tokens, lengths, slot_params, logit_scale, w_in, w_out):
        batch, toks, dim = tokens.shape
        n_slots = slot_params.shape[1]
        slots = n_slots // n_seq
        n_exp = w_in.shape[0]
        group = batch // n_model
        bc = group // CHUNKS
        bh, n = bc // 2, bc * slots
        n_fill = batch - group
        bf16, f32 = jnp.bfloat16, jnp.float32
        unit = unit_vectors(slot_params, 0)
        g = logit_scale.reshape(1)
        pos = jnp.stack([lax.axis_index("model"), lax.axis_index("seq")]).astype(jnp.int32)

        part, mz, c0 = pl.pallas_call(
            dispatch_kernel,
            grid_spec=pltpu.PrefetchScalarGridSpec(
                num_scalar_prefetch=3,
                grid=(group,),
                in_specs=[
                    pl.BlockSpec((1, toks, dim), lambda i, pos, lens, g: (pos[0] * group + i, 0, 0)),
                    pl.BlockSpec((dim, n_slots), lambda i, pos, lens, g: (0, 0)),
                ],
                out_specs=[
                    pl.BlockSpec((1, n_slots, dim), lambda i, pos, lens, g: (i, 0, 0)),
                    pl.BlockSpec((2, group, n_slots), lambda i, pos, lens, g: (0, 0, 0)),
                    pl.BlockSpec((1, toks, n_slots), lambda i, pos, lens, g: (i, 0, 0)),
                ],
            ),
            out_shape=[
                jax.ShapeDtypeStruct((group, n_slots, dim), bf16),
                jax.ShapeDtypeStruct((2, group, n_slots), f32),
                jax.ShapeDtypeStruct((group, toks, n_slots), bf16),
            ],
            compiler_params=pltpu.CompilerParams(dimension_semantics=("arbitrary",)),
            name="dispatch",
        )(pos, lengths, g, tokens, unit)

        order = np.arange(n).reshape(bc, n_exp, slots // n_exp).transpose(1, 0, 2).reshape(-1)
        perm = np.zeros((n, n), np.float32)
        perm[np.arange(n), order] = 1.0
        dims = (CHUNKS, bc, n_seq, group, n_fill, slots)
        vmem, hbm = pl.BlockSpec(memory_space=pltpu.VMEM), pl.BlockSpec(memory_space=pl.ANY)
        n_sem = n_seq + 48 * CHUNKS
        ysa, ysb, c1 = pl.pallas_call(
            functools.partial(exchange_kernel, dims, make_plan(CHUNKS, n_fill)),
            in_specs=[hbm, pl.BlockSpec(memory_space=pltpu.SMEM), vmem, hbm, vmem, hbm, hbm, vmem, vmem],
            out_specs=[hbm, hbm, hbm],
            out_shape=[
                jax.ShapeDtypeStruct((CHUNKS, RING, CORES, RING, bh, slots, dim), bf16),
                jax.ShapeDtypeStruct((CHUNKS, RING, CORES, RING, bh, slots, dim), bf16),
                jax.ShapeDtypeStruct((n_fill, toks, n_slots), bf16),
            ],
            scratch_shapes=[
                pltpu.VMEM((TOK_BUFS, toks, dim), bf16),
                pltpu.VMEM((2, toks, n_slots), bf16),
                pltpu.VMEM((group, n_slots, dim), bf16),
                pltpu.VMEM((n_seq, 2, group, n_slots), f32),
                pltpu.VMEM(w_in.shape, bf16),
                pltpu.VMEM(w_out.shape, bf16),
                pltpu.VMEM((CHUNKS, CORES, bc, RING, slots, dim), bf16),
                pltpu.VMEM((CHUNKS, bc, RING, slots, dim), bf16),
                pltpu.VMEM((CHUNKS, RING, bc, slots, dim), bf16),
                pltpu.VMEM((CHUNKS, 2, bh, slots, dim), bf16),
                pltpu.VMEM((CHUNKS, 2, bh, slots, dim), bf16),
                pltpu.VMEM((CHUNKS, 2, bc, slots, dim), bf16),
                pltpu.VMEM((CHUNKS, RING, n, dim), bf16),
                pltpu.VMEM((CHUNKS, RING, n, dim), bf16),
                pltpu.VMEM((CHUNKS, 2, n // 2, dim), bf16),
                pltpu.VMEM((CHUNKS, 2, n // 2, dim), bf16),
                pltpu.VMEM((CHUNKS, 2, n, dim), bf16),
                pltpu.VMEM((CHUNKS, RING, CORES, RING, bh, slots, dim), bf16),
                pltpu.VMEM((CHUNKS, RING, CORES, RING, bh, slots, dim), bf16),
                pltpu.SemaphoreType.DMA((TOK_BUFS,)),
                pltpu.SemaphoreType.DMA((2,)),
                pltpu.SemaphoreType.DMA((3,)),
                pltpu.SemaphoreType.DMA((2 * CHUNKS,)),
                pltpu.SemaphoreType.DMA((n_sem,)),
                pltpu.SemaphoreType.DMA((n_sem,)),
            ],
            compiler_params=pltpu.CompilerParams(collective_id=0, has_side_effects=True, vmem_limit_bytes=VMEM_LIMIT),
            name="exchange",
        )(tokens, g, unit, part, mz, w_in, w_out, jnp.asarray(perm, bf16), jnp.asarray(perm.T, bf16))

        per = group // bh
        y_grid = (RING, CHUNKS, 2)
        return pl.pallas_call(
            combine_kernel,
            grid_spec=pltpu.PrefetchScalarGridSpec(
                num_scalar_prefetch=2,
                grid=y_grid,
                in_specs=[
                    pl.BlockSpec((bh, toks, n_slots), lambda r, k, h, pos, lens: (jnp.where(r == 0, k * 2 + h, per - 1), 0, 0)),
                    pl.BlockSpec((bh, toks, n_slots), lambda r, k, h, pos, lens: (jnp.where(r == 0, 0, (r - 1) * per + k * 2 + h), 0, 0)),
                    pl.BlockSpec((1, RING, CORES, 1, bh, slots, dim), lambda r, k, h, pos, lens: (k, 0, 0, lax.rem(pos[0] + r, RING), 0, 0, 0)),
                    pl.BlockSpec((1, 1, CORES, RING, bh, slots, dim), lambda r, k, h, pos, lens: (k, lax.rem(pos[0] + r, RING), 0, 0, 0, 0, 0)),
                ],
                out_specs=pl.BlockSpec((bh, toks, dim), lambda r, k, h, pos, lens: (lax.rem(pos[0] + r, RING) * per + k * 2 + h, 0, 0)),
            ),
            out_shape=jax.ShapeDtypeStruct(tokens.shape, tokens.dtype),
            compiler_params=pltpu.CompilerParams(dimension_semantics=("arbitrary",) * 3, vmem_limit_bytes=VMEM_LIMIT),
            name="combine",
        )(pos, lengths, c0, c1, ysa, ysb)

    return jax.shard_map(local_layer, mesh=mesh, in_specs=(P("data", "seq", None), P("data"), P(), P(), P("seq", None, "model"), P("seq", "model", None)), out_specs=P("data", "seq", None), check_vma=False)
```

```python
import functools

import jax
import jax.numpy as jnp
import numpy as np
from jax import lax
from jax.experimental import pallas as pl
from jax.experimental.pallas import tpu as pltpu
from jax.sharding import PartitionSpec as P

NORM_EPS = 1e-6
NEG = -1e30
MESH = pl.DeviceIdType.MESH
CORES = 2
RING = 4
CHUNKS = 4
PAIR = 2
TOK_BUFS = 3
OUT_BUFS = 4
PLAN = (
    ("dispatch", 0), ("dispatch", 1), ("scale", 0), ("dispatch", 2), ("scale", 1), ("pair", 0), ("dispatch", 3),
    ("rsx2", 0), ("scale", 2), ("pair", 1), ("fill", 6), ("slot_in", 0), ("rsx2", 1), ("scale", 3), ("pair", 2),
    ("fill", 6), ("slot_in", 1), ("rsx2", 2), ("gy2", 0), ("pair", 3), ("fill", 6), ("slot_in", 2), ("rsx2", 3),
    ("experts", 0), ("gy2", 1), ("fill", 6), ("rsy2", 0), ("slot_in", 3), ("gy2", 2), ("fill", 6), ("slot_out", 0),
    ("experts", 1), ("gy2", 3), ("fill", 6), ("ag2", 0), ("rsy2", 1), ("experts", 2), ("experts", 3), ("ag3", 0),
    ("slot_out", 1), ("rsy2", 2), ("fill", 6), ("rsy2", 3), ("fill", 6), ("ag4", 0), ("ag2", 1), ("slot_out", 2),
    ("slot_out", 3), ("ag5", 0), ("ag3", 1), ("ag2", 2), ("finish", 0), ("ag2", 3), ("ag4", 1), ("ag3", 2),
    ("ag3", 3), ("ag5", 1), ("finish", 1), ("ag4", 2), ("ag4", 3), ("ag5", 2), ("ag5", 3), ("finish", 2),
    ("finish", 3),
)
VMEM_LIMIT = 60 * 1024 * 1024


def unit_vectors(values, axis):
    v32 = values.astype(jnp.float32)
    return (v32 * lax.rsqrt(jnp.sum(v32 * v32, axis=axis, keepdims=True) + NORM_EPS)).astype(jnp.bfloat16)


def scaled_logits(x, v, g):
    return g * jnp.dot(unit_vectors(x, 1), v, preferred_element_type=jnp.float32)


def row_softmax(logits):
    e = jnp.exp(logits - jnp.max(logits, axis=1, keepdims=True))
    return (e * (1.0 / jnp.sum(e, axis=1, keepdims=True))).astype(jnp.bfloat16)


def exchange_kernel(dims, plan, tok_hbm, len_ref, g_ref, phi_ref, win_hbm, wout_hbm, perm_ref, permt_ref,
                    ysa_hbm, ysb_hbm, c_hbm,
                    tokbuf, cbuf, unit, s_buf, mz_loc, mz_all, win, wout, sc, dr, pb, fx, sx, rx, xs, op, fy, sy, ry, ysa, ysb,
                    tok_sem, c_sem, load_sem, out_sem, send_sem, recv_sem):
    chunks, bc, n_seq, group, slots = dims
    bh, bq = bc // 2, bc // 4
    n = bc * slots
    batch, toks = tok_hbm.shape[0], tok_hbm.shape[1]
    m, s = lax.axis_index("model"), lax.axis_index("seq")
    c, x = lax.rem(s, CORES), lax.div(s, CORES)
    oc = 1 - c
    xr, xl, xo = lax.rem(x + 1, RING), lax.rem(x + RING - 1, RING), lax.rem(x + 2, RING)
    mr, ml, mo = lax.rem(m + 1, RING), lax.rem(m + RING - 1, RING), lax.rem(m + 2, RING)
    right, left = {"seq": xr * CORES + c}, {"seq": xl * CORES + c}
    up, down = {"model": mr}, {"model": ml}
    twin = {"seq": x * CORES + oc}
    row_peers = [{"seq": lax.rem(s + d, n_seq)} for d in range(1, n_seq)]
    peers = row_peers + [up, down]
    n_pairs = batch // PAIR

    def tok_copy(p):
        slot = lax.rem(p, TOK_BUFS)
        b = lax.rem(m * group + p * PAIR, batch)
        return pltpu.make_async_copy(tok_hbm.at[pl.ds(b, PAIR)], tokbuf.at[slot], tok_sem.at[slot])

    def c_copy(p):
        slot = lax.rem(p, 2)
        return pltpu.make_async_copy(cbuf.at[slot], c_hbm.at[pl.ds(p * PAIR, PAIR)], c_sem.at[slot])

    for p in range(TOK_BUFS - 1):
        tok_copy(jnp.int32(p)).start()
    loads = [pltpu.make_async_copy(a, b, load_sem.at[i]) for i, (a, b) in enumerate(((win_hbm, win), (wout_hbm, wout)))]
    for ld in loads:
        ld.start()

    barrier = pltpu.get_barrier_semaphore()
    for peer in peers:
        pl.semaphore_signal(barrier, inc=1, device_id=peer, device_id_type=MESH)
    unit[...] = unit_vectors(phi_ref[...], 0)
    mz_loc[...] = jnp.zeros_like(mz_loc)

    def next_pair(p):
        tok_copy(p).wait()

        @pl.when(p + TOK_BUFS - 1 < n_pairs)
        def _():
            tok_copy(p + TOK_BUFS - 1).start()

        @pl.when(p >= 2)
        def _():
            c_copy(p).wait()

        return lax.rem(p, TOK_BUFS), lax.rem(p, 2)

    copies = []

    def send(src, dst, dev):
        i = len(copies)
        d = pltpu.make_async_remote_copy(src_ref=src, dst_ref=dst, send_sem=send_sem.at[i], recv_sem=recv_sem.at[i], device_id=dev, device_id_type=MESH)
        d.start()
        copies.append(d)
        return d

    state = {}

    def dispatch(k):
        def one(j, carry):
            p = k * (bc // PAIR) + j
            slot, c_slot = next_pair(p)
            for q in range(PAIR):
                i = p * PAIR + q
                seq = tokbuf[slot, q]
                logits = scaled_logits(seq, unit[...], g_ref[0])
                cbuf[c_slot, q] = row_softmax(logits)
                valid = s * toks + lax.broadcasted_iota(jnp.int32, logits.shape, 0) < len_ref[m * group + i]
                masked = jnp.where(valid, logits, NEG)
                top = jnp.max(masked, axis=0, keepdims=True)
                w = jnp.where(valid, jnp.exp(masked - top), 0.0)
                mz_loc[k, 0, pl.ds(j * PAIR + q, 1), :] = top
                mz_loc[k, 1, pl.ds(j * PAIR + q, 1), :] = jnp.sum(w, axis=0, keepdims=True)
                s_buf[i] = lax.dot_general(w.astype(jnp.bfloat16), seq, (((0,), (0,)), ((), ())), preferred_element_type=jnp.float32)
            c_copy(p).start()
            return carry

        lax.fori_loop(0, bc // PAIR, one, 0)
        if k == 0:
            pl.semaphore_wait(barrier, len(peers))
        state["mz", k] = [send(mz_loc.at[k], mz_all.at[k, s], peer) for peer in row_peers]
        mz_all[k, s] = mz_loc[k]

    filled = [group // PAIR]

    def fill(count):
        lo = filled[0]
        hi = min(lo + count // PAIR, n_pairs)
        filled[0] = hi
        if hi == lo:
            return

        def one(p, carry):
            slot, c_slot = next_pair(p)
            half = toks // 2
            for q in range(PAIR):
                for r in range(0, toks, half):
                    cbuf[c_slot, q, r:r + half] = row_softmax(scaled_logits(tokbuf[slot, q, r:r + half], unit[...], g_ref[0]))
            c_copy(p).start()
            return carry

        lax.fori_loop(lo, hi, one, 0)

    def scale(k):
        for d in state["mz", k]:
            d.wait_recv()
        tops = [mz_all[k, q, 0] for q in range(n_seq)]
        top = functools.reduce(jnp.maximum, tops)
        z = functools.reduce(jnp.add, [mz_all[k, q, 1] * jnp.exp(tops[q] - top) for q in range(n_seq)])
        f = jnp.transpose(jnp.exp(mz_loc[k, 0] - top) / z)
        for j in range(bc):
            val = (s_buf[k * bc + j] * f[:, j:j + 1]).astype(jnp.bfloat16)
            for q in range(n_seq):
                sc[k, q % CORES, j, q // CORES] = val[q * slots:(q + 1) * slots]
        state["d2d", k] = send(sc.at[k, oc], dr.at[k], twin)

    def ring_send(tag, k, buf, far, r, l, f, rcv, size, rdev, ldev):
        lo, hi = pl.ds(0, size // 2), pl.ds(size // 2, size // 2)
        state[tag, k, 0] = (send(buf.at[k, far, lo], f.at[k, 0], rdev), send(buf.at[k, far, hi], f.at[k, 1], ldev))
        state[tag, k, 1] = [send(buf.at[k, r, hi], rcv.at[k, 0, hi], rdev), send(buf.at[k, l, lo], rcv.at[k, 1, lo], ldev)]

    def ring_relay(tag, k, buf, r, l, f, relay, rcv, size, rdev, ldev):
        half = size // 2
        lo, hi = pl.ds(0, half), pl.ds(half, half)
        for d in state[tag, k, 0]:
            d.wait_recv()
        relay[k, 0] = (buf[k, r, lo].astype(jnp.float32) + f[k, 0].astype(jnp.float32)).astype(jnp.bfloat16)
        relay[k, 1] = (buf[k, l, hi].astype(jnp.float32) + f[k, 1].astype(jnp.float32)).astype(jnp.bfloat16)
        state[tag, k, 1] += [send(relay.at[k, 0], rcv.at[k, 0, lo], rdev), send(relay.at[k, 1], rcv.at[k, 1, hi], ldev)]

    def ring_sum(tag, k, own, rcv):
        for d in state[tag, k, 1]:
            d.wait_recv()
        return (own.astype(jnp.float32) + rcv[k, 0].astype(jnp.float32) + rcv[k, 1].astype(jnp.float32)).astype(jnp.bfloat16)

    def pair(k):
        state["d2d", k].wait_recv()
        for q in range(RING):
            pb[k, q] = (sc[k, c, :, q].astype(jnp.float32) + dr[k, :, q].astype(jnp.float32)).astype(jnp.bfloat16)
        ring_send("x", k, pb, xo, xr, xl, fx, rx, bc, right, left)

    def rsx2(k):
        ring_relay("x", k, pb, xr, xl, fx, sx, rx, bc, right, left)

    def slot_in(k):
        val = ring_sum("x", k, pb[k, x], rx).reshape(n, -1)
        xs[k, m] = jnp.dot(perm_ref[...], val, preferred_element_type=jnp.float32).astype(jnp.bfloat16)
        state["gy", k] = [send(xs.at[k, m], xs.at[k, m], dev) for dev in (up, down)]

    def gy2(k):
        for d in state["gy", k]:
            d.wait_recv()
        lo, hi = pl.ds(0, n // 2), pl.ds(n // 2, n // 2)
        state["gy2", k] = [send(xs.at[k, ml, lo], xs.at[k, ml, lo], up), send(xs.at[k, mr, hi], xs.at[k, mr, hi], down)]

    def experts(k):
        if k == 0:
            for ld in loads:
                ld.wait()
        for d in state["gy2", k]:
            d.wait_recv()
        n_exp = win.shape[0]
        r = n // n_exp
        for e in range(n_exp):
            rows = xs[k, :, e * r:(e + 1) * r, :].reshape(RING * r, -1)
            h = jnp.dot(rows, win[e], preferred_element_type=jnp.float32)
            h = (0.5 * h * (1.0 + lax.erf(h * np.float32(np.sqrt(0.5))))).astype(jnp.bfloat16)
            o = jnp.dot(h, wout[e], preferred_element_type=jnp.float32).astype(jnp.bfloat16)
            op[k, :, e * r:(e + 1) * r, :] = o.reshape(RING, r, -1)
        ring_send("y", k, op, mo, mr, ml, fy, ry, n, up, down)

    def rsy2(k):
        ring_relay("y", k, op, mr, ml, fy, sy, ry, n, up, down)

    def slot_out(k):
        val = ring_sum("y", k, op[k, m], ry)
        val = jnp.dot(permt_ref[...], val, preferred_element_type=jnp.float32).astype(jnp.bfloat16).reshape(bc, slots, -1)
        ysa[k, x, c, m] = val[:bh]
        ysb[k, m, c, x] = val[bh:]
        a, b = ysa.at[k, x, c, m], ysb.at[k, m, c, x]
        state["g1", k] = [send(a, a, up), send(a, a, down), send(b, b, right), send(b, b, left)]

    def ag2(k):
        for d in state["g1", k]:
            d.wait_recv()
        lo, hi = pl.ds(0, bq), pl.ds(bq, bq)
        todo = [(ysa.at[k, x, c, ml, lo], up), (ysa.at[k, x, c, mr, hi], down), (ysb.at[k, m, c, xl, lo], right), (ysb.at[k, m, c, xr, hi], left)]
        state["g2", k] = [send(r, r, dev) for r, dev in todo]

    def ag3(k):
        for d in state["g2", k]:
            d.wait_recv()
        a, b = ysa.at[k, x, c], ysb.at[k, m, c]
        state["g3", k] = [send(a, a, right), send(a, a, left), send(b, b, up), send(b, b, down)]
        state["t", k] = [send(a, a, twin), send(b, b, twin)]

    def ag4(k):
        for d in state["g3", k]:
            d.wait_recv()
        lo, hi = pl.ds(0, RING // 2), pl.ds(RING // 2, RING // 2)
        todo = [(ysa.at[k, xl, c, lo], right), (ysa.at[k, xr, c, hi], left), (ysb.at[k, ml, c, lo], up), (ysb.at[k, mr, c, hi], down)]
        state["g4", k] = [send(r, r, dev) for r, dev in todo]
        state["t", k] += [send(r, r, twin) for r in (ysa.at[k, xl, c], ysa.at[k, xr, c], ysb.at[k, ml, c], ysb.at[k, mr, c])]

    def ag5(k):
        for d in state["g4", k]:
            d.wait_recv()
        state["t", k] += [send(r, r, twin) for r in (ysa.at[k, xo, c], ysb.at[k, mo, c])]

    outs = []

    def finish(k):
        for d in state["t", k]:
            d.wait_recv()
        for i, (a, b) in enumerate(((ysa, ysa_hbm), (ysb, ysb_hbm))):
            d = pltpu.make_async_copy(a.at[k], b.at[k], out_sem.at[2 * k + i])
            d.start()
            outs.append(d)

    stages = {f.__name__: f for f in (dispatch, fill, scale, pair, rsx2, slot_in, gy2, experts, rsy2, slot_out, ag2, ag3, ag4, ag5, finish)}
    for name, arg in plan:
        stages[name](arg)
    fill(batch)
    for d in outs:
        d.wait()
    for d in copies:
        d.wait_send()
    for p in range(2):
        c_copy(jnp.int32(p)).wait()


def combine_kernel(dims, c_hbm, len_ref, ysa_hbm, ysb_hbm, y_hbm, cb, ta, tb, yb, in_sem, out_sem):
    chunks, bc, n_seq, group, slots = dims
    bh = bc // 2
    toks, dim = y_hbm.shape[1], y_hbm.shape[2]
    steps = c_hbm.shape[0] // bc
    m, s = lax.axis_index("model"), lax.axis_index("seq")

    def place(i):
        return lax.rem(m + lax.div(i, chunks), RING), lax.rem(i, chunks)

    def reads(i):
        g, k = place(i)
        return [
            pltpu.make_async_copy(c_hbm.at[pl.ds(i * bc, bc)], cb.at[i], in_sem.at[i, 0]),
            pltpu.make_async_copy(ysa_hbm.at[k, :, :, g], ta.at[i], in_sem.at[i, 1]),
            pltpu.make_async_copy(ysb_hbm.at[k, g], tb.at[i], in_sem.at[i, 2]),
        ]

    def write(i):
        g, k = place(i)
        slot = lax.rem(i, OUT_BUFS)
        return pltpu.make_async_copy(yb.at[slot], y_hbm.at[pl.ds(g * group + k * bc, bc)], out_sem.at[slot])

    def start(i, carry):
        for d in reads(i):
            d.start()
        return carry

    lax.fori_loop(0, steps, start, 0)

    def one(i, carry):
        g, k = place(i)
        slot = lax.rem(i, OUT_BUFS)
        for d in reads(i):
            d.wait()

        @pl.when(i >= OUT_BUFS)
        def _():
            write(i).wait()

        for j in range(bc):
            if j < bh:
                table = ta[i, :, :, j].reshape(n_seq * slots, dim)
            else:
                table = jnp.concatenate([tb[i, q % CORES, q // CORES, j - bh] for q in range(n_seq)], axis=0)
            mixed = jnp.dot(cb[i, j], table, preferred_element_type=jnp.float32)
            valid = s * toks + lax.broadcasted_iota(jnp.int32, mixed.shape, 0) < len_ref[g * group + k * bc + j]
            yb[slot, j] = jnp.where(valid, mixed, 0.0).astype(yb.dtype)
        write(i).start()
        return carry

    lax.fori_loop(0, steps, one, 0)
    for i in range(steps - OUT_BUFS, steps):
        write(jnp.int32(i)).wait()


def solution(mesh):
    n_seq, n_model = mesh.shape["seq"], mesh.shape["model"]
    assert n_model == RING and n_seq == RING * CORES

    def local_layer(tokens, lengths, slot_params, logit_scale, w_in, w_out):
        batch, toks, dim = tokens.shape
        n_slots = slot_params.shape[1]
        slots = n_slots // n_seq
        n_exp = w_in.shape[0]
        group = batch // n_model
        bc = group // CHUNKS
        bh, n = bc // 2, bc * slots
        bf16, f32 = jnp.bfloat16, jnp.float32
        g = logit_scale.reshape(1)

        order = np.arange(n).reshape(bc, n_exp, slots // n_exp).transpose(1, 0, 2).reshape(-1)
        perm = np.zeros((n, n), np.float32)
        perm[np.arange(n), order] = 1.0
        dims = (CHUNKS, bc, n_seq, group, slots)
        rows = -(-bc // 8) * 8
        smem = pl.BlockSpec(memory_space=pltpu.SMEM)
        vmem, hbm = pl.BlockSpec(memory_space=pltpu.VMEM), pl.BlockSpec(memory_space=pl.ANY)
        n_sem = (n_seq + 48) * CHUNKS
        ysa, ysb, mix = pl.pallas_call(
            functools.partial(exchange_kernel, dims, PLAN),
            in_specs=[hbm, smem, smem, vmem, hbm, hbm, vmem, vmem],
            out_specs=[hbm, hbm, hbm],
            out_shape=[
                jax.ShapeDtypeStruct((CHUNKS, RING, CORES, RING, bh, slots, dim), bf16),
                jax.ShapeDtypeStruct((CHUNKS, RING, CORES, RING, bh, slots, dim), bf16),
                jax.ShapeDtypeStruct((batch, toks, n_slots), bf16),
            ],
            scratch_shapes=[
                pltpu.VMEM((TOK_BUFS, PAIR, toks, dim), bf16),
                pltpu.VMEM((2, PAIR, toks, n_slots), bf16),
                pltpu.VMEM((dim, n_slots), bf16),
                pltpu.VMEM((group, n_slots, dim), f32),
                pltpu.VMEM((CHUNKS, 2, rows, n_slots), f32),
                pltpu.VMEM((CHUNKS, n_seq, 2, rows, n_slots), f32),
                pltpu.VMEM(w_in.shape, bf16),
                pltpu.VMEM(w_out.shape, bf16),
                pltpu.VMEM((CHUNKS, CORES, bc, RING, slots, dim), bf16),
                pltpu.VMEM((CHUNKS, bc, RING, slots, dim), bf16),
                pltpu.VMEM((CHUNKS, RING, bc, slots, dim), bf16),
                pltpu.VMEM((CHUNKS, 2, bh, slots, dim), bf16),
                pltpu.VMEM((CHUNKS, 2, bh, slots, dim), bf16),
                pltpu.VMEM((CHUNKS, 2, bc, slots, dim), bf16),
                pltpu.VMEM((CHUNKS, RING, n, dim), bf16),
                pltpu.VMEM((CHUNKS, RING, n, dim), bf16),
                pltpu.VMEM((CHUNKS, 2, n // 2, dim), bf16),
                pltpu.VMEM((CHUNKS, 2, n // 2, dim), bf16),
                pltpu.VMEM((CHUNKS, 2, n, dim), bf16),
                pltpu.VMEM((CHUNKS, RING, CORES, RING, bh, slots, dim), bf16),
                pltpu.VMEM((CHUNKS, RING, CORES, RING, bh, slots, dim), bf16),
                pltpu.SemaphoreType.DMA((TOK_BUFS,)),
                pltpu.SemaphoreType.DMA((2,)),
                pltpu.SemaphoreType.DMA((2,)),
                pltpu.SemaphoreType.DMA((2 * CHUNKS,)),
                pltpu.SemaphoreType.DMA((n_sem,)),
                pltpu.SemaphoreType.DMA((n_sem,)),
            ],
            compiler_params=pltpu.CompilerParams(collective_id=0, has_side_effects=True, vmem_limit_bytes=VMEM_LIMIT),
            name="exchange",
        )(tokens, lengths, g, slot_params, w_in, w_out, jnp.asarray(perm, bf16), jnp.asarray(perm.T, bf16))

        steps = batch // bc
        return pl.pallas_call(
            functools.partial(combine_kernel, dims),
            in_specs=[hbm, smem, hbm, hbm],
            out_specs=hbm,
            out_shape=jax.ShapeDtypeStruct(tokens.shape, tokens.dtype),
            scratch_shapes=[
                pltpu.VMEM((steps, bc, toks, n_slots), bf16),
                pltpu.VMEM((steps, RING, CORES, bh, slots, dim), bf16),
                pltpu.VMEM((steps, CORES, RING, bh, slots, dim), bf16),
                pltpu.VMEM((OUT_BUFS, bc, toks, dim), bf16),
                pltpu.SemaphoreType.DMA((steps, 3)),
                pltpu.SemaphoreType.DMA((OUT_BUFS,)),
            ],
            compiler_params=pltpu.CompilerParams(vmem_limit_bytes=VMEM_LIMIT),
            name="combine",
        )(mix, lengths, ysa, ysb)

    return jax.shard_map(local_layer, mesh=mesh, in_specs=(P("data", "seq", None), P("data"), P(), P(), P("seq", None, "model"), P("seq", "model", None)), out_specs=P("data", "seq", None), check_vma=False)
```

```python
import functools

import jax
import jax.numpy as jnp
import numpy as np
from jax import lax
from jax.experimental import pallas as pl
from jax.experimental.pallas import tpu as pltpu
from jax.sharding import PartitionSpec as P

NORM_EPS = 1e-6
NEG = -1e30
MESH = pl.DeviceIdType.MESH
CORES = 2
RING = 4
CHUNKS = 4
PAIR = 2
TOK_BUFS = 3
OUT_BUFS = 4
PLAN = (
    ("dispatch", 0), ("dispatch", 1), ("scale", 0), ("dispatch", 2), ("pair", 0), ("scale", 1), ("pair", 1),
    ("rsx2", 0), ("scale", 2), ("dispatch", 3), ("pair", 2), ("slot_in", 0), ("rsx2", 1), ("scale", 3), ("rsx2", 2),
    ("gy2", 0), ("pair", 3), ("slot_in", 1), ("slot_in", 2), ("rsx2", 3), ("experts", 0), ("gy2", 2), ("gy2", 1),
    ("slot_in", 3), ("fill", 6), ("rsy2", 0), ("experts", 2), ("experts", 1), ("rsy2", 2), ("gy2", 3),
    ("slot_out", 0), ("fill", 6), ("rsy2", 1), ("slot_out", 2), ("experts", 3), ("ag2", 2), ("slot_out", 1),
    ("rsy2", 3), ("ag3", 2), ("ag2", 0), ("slot_out", 3), ("fill", 6), ("ag2", 1), ("ag4", 2), ("ag2", 3),
    ("ag3", 1), ("ag3", 0), ("fill", 6), ("ag3", 3), ("ag5", 2), ("fill", 6), ("ag4", 1), ("fill", 6), ("ag4", 0),
    ("fill", 6), ("ag4", 3), ("fill", 6), ("finish", 2), ("ag5", 1), ("ag5", 0), ("ag5", 3), ("finish", 3),
    ("finish", 0), ("finish", 1),
)
EXCHANGE_VMEM = 42 * 1024 * 1024
COMBINE_VMEM = 20 * 1024 * 1024


def unit_vectors(values, axis):
    v32 = values.astype(jnp.float32)
    return (v32 * lax.rsqrt(jnp.sum(v32 * v32, axis=axis, keepdims=True) + NORM_EPS)).astype(jnp.bfloat16)


def scaled_logits(x, v, g):
    return g * jnp.dot(unit_vectors(x, 1), v, preferred_element_type=jnp.float32)


def row_softmax(logits):
    e = jnp.exp(logits - jnp.max(logits, axis=1, keepdims=True))
    return (e * (1.0 / jnp.sum(e, axis=1, keepdims=True))).astype(jnp.bfloat16)


def exchange_kernel(dims, plan, tok_hbm, len_ref, g_ref, phi_ref, win_hbm, wout_hbm, perm_ref, permt_ref,
                    ysa, ysb, mix,
                    tokbuf, unit, s_buf, mz_loc, mz_all, win, wout, sc, dr, pb, fx, sx, rx, xs, op, fy, sy, ry,
                    tok_sem, load_sem, send_sem, recv_sem):
    chunks, bc, n_seq, group, slots = dims
    bh, bq = bc // 2, bc // 4
    n = bc * slots
    batch, toks = tok_hbm.shape[0], tok_hbm.shape[1]
    m, s = lax.axis_index("model"), lax.axis_index("seq")
    c, x = lax.rem(s, CORES), lax.div(s, CORES)
    oc = 1 - c
    xr, xl, xo = lax.rem(x + 1, RING), lax.rem(x + RING - 1, RING), lax.rem(x + 2, RING)
    mr, ml, mo = lax.rem(m + 1, RING), lax.rem(m + RING - 1, RING), lax.rem(m + 2, RING)
    right, left = {"seq": xr * CORES + c}, {"seq": xl * CORES + c}
    up, down = {"model": mr}, {"model": ml}
    twin = {"seq": x * CORES + oc}
    row_peers = [{"seq": lax.rem(s + d, n_seq)} for d in range(1, n_seq)]
    peers = row_peers + [up, down]
    n_pairs = batch // PAIR
    half = toks // 2

    def tok_copy(p):
        slot = lax.rem(p, TOK_BUFS)
        b = lax.rem(m * group + p * PAIR, batch)
        return pltpu.make_async_copy(tok_hbm.at[pl.ds(b, PAIR)], tokbuf.at[slot], tok_sem.at[slot])

    for p in range(TOK_BUFS - 1):
        tok_copy(jnp.int32(p)).start()
    loads = [pltpu.make_async_copy(a, b, load_sem.at[i]) for i, (a, b) in enumerate(((win_hbm, win), (wout_hbm, wout)))]
    for ld in loads:
        ld.start()

    barrier = pltpu.get_barrier_semaphore()
    for peer in peers:
        pl.semaphore_signal(barrier, inc=1, device_id=peer, device_id_type=MESH)
    unit[...] = unit_vectors(phi_ref[...], 0)
    mz_loc[...] = jnp.zeros_like(mz_loc)

    def next_pair(p):
        tok_copy(p).wait()

        @pl.when(p + TOK_BUFS - 1 < n_pairs)
        def _():
            tok_copy(p + TOK_BUFS - 1).start()

        return lax.rem(p, TOK_BUFS)

    copies = []

    def send(src, dst, dev):
        i = len(copies)
        d = pltpu.make_async_remote_copy(src_ref=src, dst_ref=dst, send_sem=send_sem.at[i], recv_sem=recv_sem.at[i], device_id=dev, device_id_type=MESH)
        d.start()
        copies.append(d)
        return d

    state = {}

    def dispatch(k):
        def one(j, carry):
            p = k * (bc // PAIR) + j
            slot = next_pair(p)
            for q in range(PAIR):
                i = p * PAIR + q
                parts = []
                for r in range(0, toks, half):
                    logits = scaled_logits(tokbuf[slot, q, r:r + half], unit[...], g_ref[0])
                    mix[i, r:r + half] = row_softmax(logits)
                    valid = s * toks + r + lax.broadcasted_iota(jnp.int32, logits.shape, 0) < len_ref[m * group + i]
                    parts.append((valid, jnp.where(valid, logits, NEG)))
                top = functools.reduce(jnp.maximum, [jnp.max(v, axis=0, keepdims=True) for _, v in parts])
                w = jnp.concatenate([jnp.where(ok, jnp.exp(v - top), 0.0) for ok, v in parts], axis=0)
                mz_loc[k, 0, pl.ds(j * PAIR + q, 1), :] = top
                mz_loc[k, 1, pl.ds(j * PAIR + q, 1), :] = jnp.sum(w, axis=0, keepdims=True)
                w = w.astype(jnp.bfloat16)
                wide = s_buf.shape[2] // 2
                for d in range(2):
                    cols = slice(d * wide, (d + 1) * wide)
                    s_buf[i, :, cols] = lax.dot_general(w, tokbuf[slot, q, :, cols], (((0,), (0,)), ((), ())), preferred_element_type=jnp.float32)
            return carry

        lax.fori_loop(0, bc // PAIR, one, 0)
        if k == 0:
            pl.semaphore_wait(barrier, len(peers))
        state["mz", k] = [send(mz_loc.at[k], mz_all.at[k, s], peer) for peer in row_peers]
        mz_all[k, s] = mz_loc[k]

    filled = [group // PAIR]

    def fill(count):
        lo = filled[0]
        hi = min(lo + count // PAIR, n_pairs)
        filled[0] = hi
        if hi == lo:
            return

        def one(p, carry):
            slot = next_pair(p)
            for q in range(PAIR):
                for r in range(0, toks, half):
                    mix[p * PAIR + q, r:r + half] = row_softmax(scaled_logits(tokbuf[slot, q, r:r + half], unit[...], g_ref[0]))
            return carry

        lax.fori_loop(lo, hi, one, 0)

    def scale(k):
        for d in state["mz", k]:
            d.wait_recv()
        tops = [mz_all[k, q, 0] for q in range(n_seq)]
        top = functools.reduce(jnp.maximum, tops)
        z = functools.reduce(jnp.add, [mz_all[k, q, 1] * jnp.exp(tops[q] - top) for q in range(n_seq)])
        f = jnp.transpose(jnp.exp(mz_loc[k, 0] - top) / z)
        for j in range(bc):
            val = (s_buf[k * bc + j] * f[:, j:j + 1]).astype(jnp.bfloat16)
            for q in range(n_seq):
                sc[k, q % CORES, j, q // CORES] = val[q * slots:(q + 1) * slots]
        state["d2d", k] = send(sc.at[k, oc], dr.at[k], twin)

    def ring_send(tag, k, buf, far, r, l, f, rcv, size, rdev, ldev):
        lo, hi = pl.ds(0, size // 2), pl.ds(size // 2, size // 2)
        state[tag, k, 0] = (send(buf.at[k, far, lo], f.at[k, 0], rdev), send(buf.at[k, far, hi], f.at[k, 1], ldev))
        state[tag, k, 1] = [send(buf.at[k, r, hi], rcv.at[k, 0, hi], rdev), send(buf.at[k, l, lo], rcv.at[k, 1, lo], ldev)]

    def ring_relay(tag, k, buf, r, l, f, relay, rcv, size, rdev, ldev):
        half = size // 2
        lo, hi = pl.ds(0, half), pl.ds(half, half)
        for d in state[tag, k, 0]:
            d.wait_recv()
        relay[k, 0] = (buf[k, r, lo].astype(jnp.float32) + f[k, 0].astype(jnp.float32)).astype(jnp.bfloat16)
        relay[k, 1] = (buf[k, l, hi].astype(jnp.float32) + f[k, 1].astype(jnp.float32)).astype(jnp.bfloat16)
        state[tag, k, 1] += [send(relay.at[k, 0], rcv.at[k, 0, lo], rdev), send(relay.at[k, 1], rcv.at[k, 1, hi], ldev)]

    def ring_sum(tag, k, own, rcv):
        for d in state[tag, k, 1]:
            d.wait_recv()
        return (own.astype(jnp.float32) + rcv[k, 0].astype(jnp.float32) + rcv[k, 1].astype(jnp.float32)).astype(jnp.bfloat16)

    def pair(k):
        state["d2d", k].wait_recv()
        for q in range(RING):
            pb[k, q] = (sc[k, c, :, q].astype(jnp.float32) + dr[k, :, q].astype(jnp.float32)).astype(jnp.bfloat16)
        ring_send("x", k, pb, xo, xr, xl, fx, rx, bc, right, left)

    def rsx2(k):
        ring_relay("x", k, pb, xr, xl, fx, sx, rx, bc, right, left)

    def slot_in(k):
        val = ring_sum("x", k, pb[k, x], rx).reshape(n, -1)
        xs[k, m] = jnp.dot(perm_ref[...], val, preferred_element_type=jnp.float32).astype(jnp.bfloat16)
        state["gy", k] = [send(xs.at[k, m], xs.at[k, m], dev) for dev in (up, down)]

    def gy2(k):
        for d in state["gy", k]:
            d.wait_recv()
        lo, hi = pl.ds(0, n // 2), pl.ds(n // 2, n // 2)
        state["gy2", k] = [send(xs.at[k, ml, lo], xs.at[k, ml, lo], up), send(xs.at[k, mr, hi], xs.at[k, mr, hi], down)]

    def experts(k):
        while loads:
            loads.pop().wait()
        for d in state["gy2", k]:
            d.wait_recv()
        n_exp = win.shape[0]
        r = n // n_exp
        for e in range(n_exp):
            rows = xs[k, :, e * r:(e + 1) * r, :].reshape(RING * r, -1)
            h = jnp.dot(rows, win[e], preferred_element_type=jnp.float32)
            h = (0.5 * h * (1.0 + lax.erf(h * np.float32(np.sqrt(0.5))))).astype(jnp.bfloat16)
            o = jnp.dot(h, wout[e], preferred_element_type=jnp.float32).astype(jnp.bfloat16)
            op[k, :, e * r:(e + 1) * r, :] = o.reshape(RING, r, -1)
        ring_send("y", k, op, mo, mr, ml, fy, ry, n, up, down)

    def rsy2(k):
        ring_relay("y", k, op, mr, ml, fy, sy, ry, n, up, down)

    def slot_out(k):
        val = ring_sum("y", k, op[k, m], ry)
        val = jnp.dot(permt_ref[...], val, preferred_element_type=jnp.float32).astype(jnp.bfloat16).reshape(bc, slots, -1)
        ysa[k, x, c, m] = val[:bh]
        ysb[k, m, c, x] = val[bh:]
        a, b = ysa.at[k, x, c, m], ysb.at[k, m, c, x]
        state["g1", k] = [send(a, a, up), send(a, a, down), send(b, b, right), send(b, b, left)]

    def ag2(k):
        for d in state["g1", k]:
            d.wait_recv()
        lo, hi = pl.ds(0, bq), pl.ds(bq, bq)
        todo = [(ysa.at[k, x, c, ml, lo], up), (ysa.at[k, x, c, mr, hi], down), (ysb.at[k, m, c, xl, lo], right), (ysb.at[k, m, c, xr, hi], left)]
        state["g2", k] = [send(r, r, dev) for r, dev in todo]

    def ag3(k):
        for d in state["g2", k]:
            d.wait_recv()
        a, b = ysa.at[k, x, c], ysb.at[k, m, c]
        state["g3", k] = [send(a, a, right), send(a, a, left), send(b, b, up), send(b, b, down)]
        state["t", k] = [send(a, a, twin), send(b, b, twin)]

    def ag4(k):
        for d in state["g3", k]:
            d.wait_recv()
        lo, hi = pl.ds(0, RING // 2), pl.ds(RING // 2, RING // 2)
        todo = [(ysa.at[k, xl, c, lo], right), (ysa.at[k, xr, c, hi], left), (ysb.at[k, ml, c, lo], up), (ysb.at[k, mr, c, hi], down)]
        state["g4", k] = [send(r, r, dev) for r, dev in todo]
        state["t", k] += [send(r, r, twin) for r in (ysa.at[k, xl, c], ysa.at[k, xr, c], ysb.at[k, ml, c], ysb.at[k, mr, c])]

    def ag5(k):
        for d in state["g4", k]:
            d.wait_recv()
        state["t", k] += [send(r, r, twin) for r in (ysa.at[k, xo, c], ysb.at[k, mo, c])]

    def finish(k):
        for d in state["t", k]:
            d.wait_recv()

    stages = {f.__name__: f for f in (dispatch, fill, scale, pair, rsx2, slot_in, gy2, experts, rsy2, slot_out, ag2, ag3, ag4, ag5, finish)}
    for name, arg in plan:
        stages[name](arg)
    fill(batch)
    for d in copies:
        d.wait_send()


def combine_kernel(dims, mix, len_ref, ysa, ysb, y_hbm, yb, out_sem):
    chunks, bc, n_seq, group, slots = dims
    bh = bc // 2
    toks, dim = y_hbm.shape[1], y_hbm.shape[2]
    steps = mix.shape[0] // bc
    m, s = lax.axis_index("model"), lax.axis_index("seq")

    def place(i):
        return lax.rem(m + lax.div(i, chunks), RING), lax.rem(i, chunks)

    def write(i):
        g, k = place(i)
        slot = lax.rem(i, OUT_BUFS)
        return pltpu.make_async_copy(yb.at[slot], y_hbm.at[pl.ds(g * group + k * bc, bc)], out_sem.at[slot])

    def one(i, carry):
        g, k = place(i)
        slot = lax.rem(i, OUT_BUFS)

        @pl.when(i >= OUT_BUFS)
        def _():
            write(i).wait()

        for j in range(bc):
            if j < bh:
                table = ysa[k, :, :, g, j].reshape(n_seq * slots, dim)
            else:
                table = jnp.concatenate([ysb[k, g, q % CORES, q // CORES, j - bh] for q in range(n_seq)], axis=0)
            mixed = jnp.dot(mix[i * bc + j], table, preferred_element_type=jnp.float32)
            valid = s * toks + lax.broadcasted_iota(jnp.int32, mixed.shape, 0) < len_ref[g * group + k * bc + j]
            yb[slot, j] = jnp.where(valid, mixed, 0.0).astype(yb.dtype)
        write(i).start()
        return carry

    lax.fori_loop(0, steps, one, 0)
    for i in range(steps - OUT_BUFS, steps):
        write(jnp.int32(i)).wait()


def solution(mesh):
    n_seq, n_model = mesh.shape["seq"], mesh.shape["model"]
    assert n_model == RING and n_seq == RING * CORES

    def local_layer(tokens, lengths, slot_params, logit_scale, w_in, w_out):
        batch, toks, dim = tokens.shape
        n_slots = slot_params.shape[1]
        slots = n_slots // n_seq
        n_exp = w_in.shape[0]
        group = batch // n_model
        bc = group // CHUNKS
        bh, n = bc // 2, bc * slots
        bf16, f32 = jnp.bfloat16, jnp.float32
        g = logit_scale.reshape(1)

        order = np.arange(n).reshape(bc, n_exp, slots // n_exp).transpose(1, 0, 2).reshape(-1)
        perm = np.zeros((n, n), np.float32)
        perm[np.arange(n), order] = 1.0
        dims = (CHUNKS, bc, n_seq, group, slots)
        rows = -(-bc // 8) * 8
        smem = pl.BlockSpec(memory_space=pltpu.SMEM)
        vmem, hbm = pl.BlockSpec(memory_space=pltpu.VMEM), pl.BlockSpec(memory_space=pl.ANY)
        n_sem = (n_seq + 48) * CHUNKS
        ysa, ysb, mix = pl.pallas_call(
            functools.partial(exchange_kernel, dims, PLAN),
            in_specs=[hbm, smem, smem, vmem, hbm, hbm, vmem, vmem],
            out_specs=[vmem, vmem, vmem],
            out_shape=[
                pltpu.VMEM((CHUNKS, RING, CORES, RING, bh, slots, dim), bf16),
                pltpu.VMEM((CHUNKS, RING, CORES, RING, bh, slots, dim), bf16),
                pltpu.VMEM((batch, toks, n_slots), bf16),
            ],
            scratch_shapes=[
                pltpu.VMEM((TOK_BUFS, PAIR, toks, dim), bf16),
                pltpu.VMEM((dim, n_slots), bf16),
                pltpu.VMEM((group, n_slots, dim), f32),
                pltpu.VMEM((CHUNKS, 2, rows, n_slots), f32),
                pltpu.VMEM((CHUNKS, n_seq, 2, rows, n_slots), f32),
                pltpu.VMEM(w_in.shape, bf16),
                pltpu.VMEM(w_out.shape, bf16),
                pltpu.VMEM((CHUNKS, CORES, bc, RING, slots, dim), bf16),
                pltpu.VMEM((CHUNKS, bc, RING, slots, dim), bf16),
                pltpu.VMEM((CHUNKS, RING, bc, slots, dim), bf16),
                pltpu.VMEM((CHUNKS, 2, bh, slots, dim), bf16),
                pltpu.VMEM((CHUNKS, 2, bh, slots, dim), bf16),
                pltpu.VMEM((CHUNKS, 2, bc, slots, dim), bf16),
                pltpu.VMEM((CHUNKS, RING, n, dim), bf16),
                pltpu.VMEM((CHUNKS, RING, n, dim), bf16),
                pltpu.VMEM((CHUNKS, 2, n // 2, dim), bf16),
                pltpu.VMEM((CHUNKS, 2, n // 2, dim), bf16),
                pltpu.VMEM((CHUNKS, 2, n, dim), bf16),
                pltpu.SemaphoreType.DMA((TOK_BUFS,)),
                pltpu.SemaphoreType.DMA((2,)),
                pltpu.SemaphoreType.DMA((n_sem,)),
                pltpu.SemaphoreType.DMA((n_sem,)),
            ],
            compiler_params=pltpu.CompilerParams(collective_id=0, has_side_effects=True, vmem_limit_bytes=EXCHANGE_VMEM),
            name="exchange",
        )(tokens, lengths, g, slot_params, w_in, w_out, jnp.asarray(perm, bf16), jnp.asarray(perm.T, bf16))

        mix, ysa, ysb = (pltpu.with_memory_space_constraint(a, pltpu.VMEM) for a in (mix, ysa, ysb))
        return pl.pallas_call(
            functools.partial(combine_kernel, dims),
            in_specs=[vmem, smem, vmem, vmem],
            out_specs=hbm,
            out_shape=jax.ShapeDtypeStruct(tokens.shape, tokens.dtype),
            scratch_shapes=[
                pltpu.VMEM((OUT_BUFS, bc, toks, dim), bf16),
                pltpu.SemaphoreType.DMA((OUT_BUFS,)),
            ],
            compiler_params=pltpu.CompilerParams(vmem_limit_bytes=COMBINE_VMEM),
            name="combine",
        )(mix, lengths, ysa, ysb)

    return jax.shard_map(local_layer, mesh=mesh, in_specs=(P("data", "seq", None), P("data"), P(), P(), P("seq", None, "model"), P("seq", "model", None)), out_specs=P("data", "seq", None), check_vma=False)
```

```python
import functools

import jax
import jax.numpy as jnp
import numpy as np
from jax import lax
from jax.experimental import pallas as pl
from jax.experimental.pallas import tpu as pltpu
from jax.sharding import PartitionSpec as P

NORM_EPS = 1e-6
NEG = -1e30
MESH = pl.DeviceIdType.MESH
CORES = 2
RING = 4
CHUNKS = 4
PAIR = 2
TOK_BUFS = 3
OUT_BUFS = 4
PLAN = (
    ("dispatch", 0), ("dispatch", 1), ("scale", 0), ("dispatch", 2), ("pair", 0), ("scale", 1), ("pair", 1),
    ("dispatch", 3), ("rsx2", 1), ("rsx2", 0), ("scale", 2), ("pair", 2), ("scale", 3), ("slot_in", 1), ("pair", 3),
    ("slot_in", 0), ("rsx2", 2), ("rsx2", 3), ("gy2", 1), ("gy2", 0), ("slot_in", 2), ("slot_in", 3),
    ("experts", 1), ("fill", 6), ("gy2", 2), ("experts", 0), ("gy2", 3), ("rsy2", 1), ("fill", 6), ("rsy2", 0),
    ("experts", 2), ("experts", 3), ("slot_out", 1), ("fill", 6), ("rsy2", 2), ("rsy2", 3), ("ag2", 1),
    ("slot_out", 0), ("slot_out", 2), ("slot_out", 3), ("ag3", 1), ("ag2", 2), ("fill", 6), ("ag2", 3), ("ag2", 0),
    ("ag4", 1), ("ag3", 2), ("ag3", 3), ("ag3", 0), ("fill", 18), ("agt", 1), ("ag5", 1), ("ag4", 3), ("agt", 3),
    ("ag4", 0), ("agt", 0), ("ag4", 2), ("finish", 1), ("agt", 2), ("fill", 6), ("ag5", 3), ("ag5", 0), ("ag5", 2),
    ("finish", 3), ("finish", 0), ("finish", 2),
)
EXCHANGE_VMEM = 42 * 1024 * 1024
COMBINE_VMEM = 20 * 1024 * 1024


def unit_vectors(values, axis):
    v32 = values.astype(jnp.float32)
    return (v32 * lax.rsqrt(jnp.sum(v32 * v32, axis=axis, keepdims=True) + NORM_EPS)).astype(jnp.bfloat16)


def scaled_logits(x, v, g):
    return g * jnp.dot(unit_vectors(x, 1), v, preferred_element_type=jnp.float32)


def row_softmax(logits):
    e = jnp.exp(logits - jnp.max(logits, axis=1, keepdims=True))
    return (e * (1.0 / jnp.sum(e, axis=1, keepdims=True))).astype(jnp.bfloat16)


def exchange_kernel(dims, plan, tok_hbm, len_ref, g_ref, phi_ref, win_hbm, wout_hbm, perm_ref, permt_ref,
                    ysa, ysb, mix,
                    tokbuf, unit, s_buf, mz_loc, mz_all, win, wout, sc, dr, pb, fx, sx, rx, xs, op, fy, sy, ry,
                    tok_sem, load_sem, send_sem, recv_sem):
    chunks, bc, n_seq, group, slots = dims
    bh, bq = bc // 2, bc // 4
    n = bc * slots
    batch, toks = tok_hbm.shape[0], tok_hbm.shape[1]
    m, s = lax.axis_index("model"), lax.axis_index("seq")
    c, x = lax.rem(s, CORES), lax.div(s, CORES)
    oc = 1 - c
    xr, xl, xo = lax.rem(x + 1, RING), lax.rem(x + RING - 1, RING), lax.rem(x + 2, RING)
    mr, ml, mo = lax.rem(m + 1, RING), lax.rem(m + RING - 1, RING), lax.rem(m + 2, RING)
    right, left = {"seq": xr * CORES + c}, {"seq": xl * CORES + c}
    up, down = {"model": mr}, {"model": ml}
    twin = {"seq": x * CORES + oc}
    row_peers = [{"seq": lax.rem(s + d, n_seq)} for d in range(1, n_seq)]
    peers = row_peers + [up, down]
    n_pairs = batch // PAIR
    half = toks // 2

    def tok_copy(p):
        slot = lax.rem(p, TOK_BUFS)
        b = lax.rem(m * group + p * PAIR, batch)
        return pltpu.make_async_copy(tok_hbm.at[pl.ds(b, PAIR)], tokbuf.at[slot], tok_sem.at[slot])

    for p in range(TOK_BUFS - 1):
        tok_copy(jnp.int32(p)).start()
    loads = [pltpu.make_async_copy(a, b, load_sem.at[i]) for i, (a, b) in enumerate(((win_hbm, win), (wout_hbm, wout)))]
    for ld in loads:
        ld.start()

    barrier = pltpu.get_barrier_semaphore()
    for peer in peers:
        pl.semaphore_signal(barrier, inc=1, device_id=peer, device_id_type=MESH)
    unit[...] = unit_vectors(phi_ref[...], 0)
    mz_loc[...] = jnp.zeros_like(mz_loc)

    def next_pair(p):
        tok_copy(p).wait()

        @pl.when(p + TOK_BUFS - 1 < n_pairs)
        def _():
            tok_copy(p + TOK_BUFS - 1).start()

        return lax.rem(p, TOK_BUFS)

    copies = []

    def send(src, dst, dev):
        i = len(copies)
        d = pltpu.make_async_remote_copy(src_ref=src, dst_ref=dst, send_sem=send_sem.at[i], recv_sem=recv_sem.at[i], device_id=dev, device_id_type=MESH)
        d.start()
        copies.append(d)
        return d

    state = {}

    def dispatch(k):
        def one(j, carry):
            p = k * (bc // PAIR) + j
            slot = next_pair(p)
            for q in range(PAIR):
                i = p * PAIR + q
                parts = []
                for r in range(0, toks, half):
                    logits = scaled_logits(tokbuf[slot, q, r:r + half], unit[...], g_ref[0])
                    mix[i, r:r + half] = row_softmax(logits)
                    valid = s * toks + r + lax.broadcasted_iota(jnp.int32, logits.shape, 0) < len_ref[m * group + i]
                    parts.append((valid, jnp.where(valid, logits, NEG)))
                top = functools.reduce(jnp.maximum, [jnp.max(v, axis=0, keepdims=True) for _, v in parts])
                w = jnp.concatenate([jnp.where(ok, jnp.exp(v - top), 0.0) for ok, v in parts], axis=0)
                mz_loc[k, 0, pl.ds(j * PAIR + q, 1), :] = top
                mz_loc[k, 1, pl.ds(j * PAIR + q, 1), :] = jnp.sum(w, axis=0, keepdims=True)
                w = w.astype(jnp.bfloat16)
                wide = s_buf.shape[2] // 2
                for d in range(2):
                    cols = slice(d * wide, (d + 1) * wide)
                    s_buf[i, :, cols] = lax.dot_general(w, tokbuf[slot, q, :, cols], (((0,), (0,)), ((), ())), preferred_element_type=jnp.float32)
            return carry

        lax.fori_loop(0, bc // PAIR, one, 0)
        if k == 0:
            pl.semaphore_wait(barrier, len(peers))
        state["mz", k] = [send(mz_loc.at[k], mz_all.at[k, s], peer) for peer in row_peers]
        mz_all[k, s] = mz_loc[k]

    filled = [group // PAIR]

    def fill(count):
        lo = filled[0]
        hi = min(lo + count // PAIR, n_pairs)
        filled[0] = hi
        if hi == lo:
            return

        def one(p, carry):
            slot = next_pair(p)
            for q in range(PAIR):
                for r in range(0, toks, half):
                    mix[p * PAIR + q, r:r + half] = row_softmax(scaled_logits(tokbuf[slot, q, r:r + half], unit[...], g_ref[0]))
            return carry

        lax.fori_loop(lo, hi, one, 0)

    def scale(k):
        for d in state["mz", k]:
            d.wait_recv()
        tops = [mz_all[k, q, 0] for q in range(n_seq)]
        top = functools.reduce(jnp.maximum, tops)
        z = functools.reduce(jnp.add, [mz_all[k, q, 1] * jnp.exp(tops[q] - top) for q in range(n_seq)])
        f = jnp.transpose(jnp.exp(mz_loc[k, 0] - top) / z)
        for j in range(bc):
            val = (s_buf[k * bc + j] * f[:, j:j + 1]).astype(jnp.bfloat16)
            for q in range(n_seq):
                sc[k, q % CORES, j, q // CORES] = val[q * slots:(q + 1) * slots]
        state["d2d", k] = send(sc.at[k, oc], dr.at[k], twin)

    def ring_send(tag, k, buf, far, r, l, f, rcv, size, rdev, ldev):
        lo, hi = pl.ds(0, size // 2), pl.ds(size // 2, size // 2)
        state[tag, k, 0] = (send(buf.at[k, far, lo], f.at[k, 0], rdev), send(buf.at[k, far, hi], f.at[k, 1], ldev))
        state[tag, k, 1] = [send(buf.at[k, r, hi], rcv.at[k, 0, hi], rdev), send(buf.at[k, l, lo], rcv.at[k, 1, lo], ldev)]

    def ring_relay(tag, k, buf, r, l, f, relay, rcv, size, rdev, ldev):
        half = size // 2
        lo, hi = pl.ds(0, half), pl.ds(half, half)
        for d in state[tag, k, 0]:
            d.wait_recv()
        relay[k, 0] = (buf[k, r, lo].astype(jnp.float32) + f[k, 0].astype(jnp.float32)).astype(jnp.bfloat16)
        relay[k, 1] = (buf[k, l, hi].astype(jnp.float32) + f[k, 1].astype(jnp.float32)).astype(jnp.bfloat16)
        state[tag, k, 1] += [send(relay.at[k, 0], rcv.at[k, 0, lo], rdev), send(relay.at[k, 1], rcv.at[k, 1, hi], ldev)]

    def ring_sum(tag, k, own, rcv):
        for d in state[tag, k, 1]:
            d.wait_recv()
        return (own.astype(jnp.float32) + rcv[k, 0].astype(jnp.float32) + rcv[k, 1].astype(jnp.float32)).astype(jnp.bfloat16)

    def pair(k):
        state["d2d", k].wait_recv()
        for q in range(RING):
            pb[k, q] = (sc[k, c, :, q].astype(jnp.float32) + dr[k, :, q].astype(jnp.float32)).astype(jnp.bfloat16)
        ring_send("x", k, pb, xo, xr, xl, fx, rx, bc, right, left)

    def rsx2(k):
        ring_relay("x", k, pb, xr, xl, fx, sx, rx, bc, right, left)

    def relayed_first(tag, k, todo):
        state[tag, k] = [send(first, first, dev) for first, _, dev in todo]
        state[tag + "r", k] = [send(second, second, dev) for _, second, dev in todo]

    def slot_in(k):
        val = ring_sum("x", k, pb[k, x], rx).reshape(n, -1)
        xs[k, m] = jnp.dot(perm_ref[...], val, preferred_element_type=jnp.float32).astype(jnp.bfloat16)
        lo, hi = xs.at[k, m, pl.ds(0, n // 2)], xs.at[k, m, pl.ds(n // 2, n // 2)]
        relayed_first("gy", k, [(lo, hi, up), (hi, lo, down)])

    def gy2(k):
        for d in state["gy", k]:
            d.wait_recv()
        lo, hi = pl.ds(0, n // 2), pl.ds(n // 2, n // 2)
        state["gy2", k] = [send(xs.at[k, ml, lo], xs.at[k, ml, lo], up), send(xs.at[k, mr, hi], xs.at[k, mr, hi], down)]

    def experts(k):
        while loads:
            loads.pop().wait()
        for d in state["gyr", k] + state["gy2", k]:
            d.wait_recv()
        n_exp = win.shape[0]
        r = n // n_exp
        for e in range(n_exp):
            rows = xs[k, :, e * r:(e + 1) * r, :].reshape(RING * r, -1)
            h = jnp.dot(rows, win[e], preferred_element_type=jnp.float32)
            h = (0.5 * h * (1.0 + lax.erf(h * np.float32(np.sqrt(0.5))))).astype(jnp.bfloat16)
            o = jnp.dot(h, wout[e], preferred_element_type=jnp.float32).astype(jnp.bfloat16)
            op[k, :, e * r:(e + 1) * r, :] = o.reshape(RING, r, -1)
        ring_send("y", k, op, mo, mr, ml, fy, ry, n, up, down)

    def rsy2(k):
        ring_relay("y", k, op, mr, ml, fy, sy, ry, n, up, down)

    def slot_out(k):
        val = ring_sum("y", k, op[k, m], ry)
        val = jnp.dot(permt_ref[...], val, preferred_element_type=jnp.float32).astype(jnp.bfloat16).reshape(bc, slots, -1)
        ysa[k, x, c, m] = val[:bh]
        ysb[k, m, c, x] = val[bh:]
        lo, hi = pl.ds(0, bq), pl.ds(bq, bq)
        a_lo, a_hi, b_lo, b_hi = ysa.at[k, x, c, m, lo], ysa.at[k, x, c, m, hi], ysb.at[k, m, c, x, lo], ysb.at[k, m, c, x, hi]
        relayed_first("g1", k, [(a_lo, a_hi, up), (a_hi, a_lo, down), (b_lo, b_hi, right), (b_hi, b_lo, left)])

    def ag2(k):
        for d in state["g1", k]:
            d.wait_recv()
        lo, hi = pl.ds(0, bq), pl.ds(bq, bq)
        todo = [(ysa.at[k, x, c, ml, lo], up), (ysa.at[k, x, c, mr, hi], down), (ysb.at[k, m, c, xl, lo], right), (ysb.at[k, m, c, xr, hi], left)]
        state["g2", k] = [send(r, r, dev) for r, dev in todo]

    def ag3(k):
        for d in state["g1r", k] + state["g2", k]:
            d.wait_recv()
        a, b = ysa.at[k, x, c], ysb.at[k, m, c]
        lo, hi = pl.ds(0, RING // 2), pl.ds(RING // 2, RING // 2)
        a_lo, a_hi, b_lo, b_hi = ysa.at[k, x, c, lo], ysa.at[k, x, c, hi], ysb.at[k, m, c, lo], ysb.at[k, m, c, hi]
        relayed_first("g3", k, [(a_lo, a_hi, right), (a_hi, a_lo, left), (b_lo, b_hi, up), (b_hi, b_lo, down)])
        state["t", k] = [send(a, a, twin), send(b, b, twin)]

    def ag4(k):
        for d in state["g3", k]:
            d.wait_recv()
        lo, hi = pl.ds(0, RING // 2), pl.ds(RING // 2, RING // 2)
        todo = [(ysa.at[k, xl, c, lo], right), (ysa.at[k, xr, c, hi], left), (ysb.at[k, ml, c, lo], up), (ysb.at[k, mr, c, hi], down)]
        state["g4", k] = [send(r, r, dev) for r, dev in todo]

    def agt(k):
        for d in state["g3r", k]:
            d.wait_recv()
        state["t", k] += [send(r, r, twin) for r in (ysa.at[k, xl, c], ysa.at[k, xr, c], ysb.at[k, ml, c], ysb.at[k, mr, c])]

    def ag5(k):
        for d in state["g4", k]:
            d.wait_recv()
        state["t", k] += [send(r, r, twin) for r in (ysa.at[k, xo, c], ysb.at[k, mo, c])]

    def finish(k):
        for d in state["t", k]:
            d.wait_recv()

    stages = {f.__name__: f for f in (dispatch, fill, scale, pair, rsx2, slot_in, gy2, experts, rsy2, slot_out, ag2, ag3, ag4, agt, ag5, finish)}
    for name, arg in plan:
        stages[name](arg)
    fill(batch)
    for d in copies:
        d.wait_send()


def combine_kernel(dims, mix, len_ref, ysa, ysb, y_hbm, yb, out_sem):
    chunks, bc, n_seq, group, slots = dims
    bh = bc // 2
    toks, dim = y_hbm.shape[1], y_hbm.shape[2]
    steps = mix.shape[0] // bc
    m, s = lax.axis_index("model"), lax.axis_index("seq")

    def place(i):
        return lax.rem(m + lax.div(i, chunks), RING), lax.rem(i, chunks)

    def write(i, j):
        g, k = place(i)
        slot = lax.rem(i, OUT_BUFS)
        return pltpu.make_async_copy(yb.at[slot, j], y_hbm.at[g * group + k * bc + j], out_sem.at[slot, j])

    def one(i, carry):
        g, k = place(i)
        slot = lax.rem(i, OUT_BUFS)

        @pl.when(i >= OUT_BUFS)
        def _():
            for j in range(bc):
                write(i, j).wait()

        for j in range(bc):
            if j < bh:
                table = ysa[k, :, :, g, j].reshape(n_seq * slots, dim)
            else:
                table = jnp.concatenate([ysb[k, g, q % CORES, q // CORES, j - bh] for q in range(n_seq)], axis=0)
            mixed = jnp.dot(mix[i * bc + j], table, preferred_element_type=jnp.float32)
            valid = s * toks + lax.broadcasted_iota(jnp.int32, mixed.shape, 0) < len_ref[g * group + k * bc + j]
            yb[slot, j] = jnp.where(valid, mixed, 0.0).astype(yb.dtype)
            write(i, j).start()
        return carry

    lax.fori_loop(0, steps, one, 0)
    for i in range(steps - OUT_BUFS, steps):
        for j in range(bc):
            write(jnp.int32(i), j).wait()


def solution(mesh):
    n_seq, n_model = mesh.shape["seq"], mesh.shape["model"]
    assert n_model == RING and n_seq == RING * CORES

    def local_layer(tokens, lengths, slot_params, logit_scale, w_in, w_out):
        batch, toks, dim = tokens.shape
        n_slots = slot_params.shape[1]
        slots = n_slots // n_seq
        n_exp = w_in.shape[0]
        group = batch // n_model
        bc = group // CHUNKS
        bh, n = bc // 2, bc * slots
        bf16, f32 = jnp.bfloat16, jnp.float32
        g = logit_scale.reshape(1)

        order = np.arange(n).reshape(bc, n_exp, slots // n_exp).transpose(1, 0, 2).reshape(-1)
        perm = np.zeros((n, n), np.float32)
        perm[np.arange(n), order] = 1.0
        dims = (CHUNKS, bc, n_seq, group, slots)
        rows = -(-bc // 8) * 8
        smem = pl.BlockSpec(memory_space=pltpu.SMEM)
        vmem, hbm = pl.BlockSpec(memory_space=pltpu.VMEM), pl.BlockSpec(memory_space=pl.ANY)
        n_sem = (n_seq + 56) * CHUNKS
        ysa, ysb, mix = pl.pallas_call(
            functools.partial(exchange_kernel, dims, PLAN),
            in_specs=[hbm, smem, smem, vmem, hbm, hbm, vmem, vmem],
            out_specs=[vmem, vmem, vmem],
            out_shape=[
                pltpu.VMEM((CHUNKS, RING, CORES, RING, bh, slots, dim), bf16),
                pltpu.VMEM((CHUNKS, RING, CORES, RING, bh, slots, dim), bf16),
                pltpu.VMEM((batch, toks, n_slots), bf16),
            ],
            scratch_shapes=[
                pltpu.VMEM((TOK_BUFS, PAIR, toks, dim), bf16),
                pltpu.VMEM((dim, n_slots), bf16),
                pltpu.VMEM((group, n_slots, dim), f32),
                pltpu.VMEM((CHUNKS, 2, rows, n_slots), f32),
                pltpu.VMEM((CHUNKS, n_seq, 2, rows, n_slots), f32),
                pltpu.VMEM(w_in.shape, bf16),
                pltpu.VMEM(w_out.shape, bf16),
                pltpu.VMEM((CHUNKS, CORES, bc, RING, slots, dim), bf16),
                pltpu.VMEM((CHUNKS, bc, RING, slots, dim), bf16),
                pltpu.VMEM((CHUNKS, RING, bc, slots, dim), bf16),
                pltpu.VMEM((CHUNKS, 2, bh, slots, dim), bf16),
                pltpu.VMEM((CHUNKS, 2, bh, slots, dim), bf16),
                pltpu.VMEM((CHUNKS, 2, bc, slots, dim), bf16),
                pltpu.VMEM((CHUNKS, RING, n, dim), bf16),
                pltpu.VMEM((CHUNKS, RING, n, dim), bf16),
                pltpu.VMEM((CHUNKS, 2, n // 2, dim), bf16),
                pltpu.VMEM((CHUNKS, 2, n // 2, dim), bf16),
                pltpu.VMEM((CHUNKS, 2, n, dim), bf16),
                pltpu.SemaphoreType.DMA((TOK_BUFS,)),
                pltpu.SemaphoreType.DMA((2,)),
                pltpu.SemaphoreType.DMA((n_sem,)),
                pltpu.SemaphoreType.DMA((n_sem,)),
            ],
            compiler_params=pltpu.CompilerParams(collective_id=0, has_side_effects=True, vmem_limit_bytes=EXCHANGE_VMEM),
            name="exchange",
        )(tokens, lengths, g, slot_params, w_in, w_out, jnp.asarray(perm, bf16), jnp.asarray(perm.T, bf16))

        mix, ysa, ysb = (pltpu.with_memory_space_constraint(a, pltpu.VMEM) for a in (mix, ysa, ysb))
        return pl.pallas_call(
            functools.partial(combine_kernel, dims),
            in_specs=[vmem, smem, vmem, vmem],
            out_specs=hbm,
            out_shape=jax.ShapeDtypeStruct(tokens.shape, tokens.dtype),
            scratch_shapes=[
                pltpu.VMEM((OUT_BUFS, bc, toks, dim), bf16),
                pltpu.SemaphoreType.DMA((OUT_BUFS, bc)),
            ],
            compiler_params=pltpu.CompilerParams(vmem_limit_bytes=COMBINE_VMEM),
            name="combine",
        )(mix, lengths, ysa, ysb)

    return jax.shard_map(local_layer, mesh=mesh, in_specs=(P("data", "seq", None), P("data"), P(), P(), P("seq", None, "model"), P("seq", "model", None)), out_specs=P("data", "seq", None), check_vma=False)
```
